32 devices in a mesh: dp: 1 (over z), tp: 4 (over y), sp: 8 (over x, core).
Axes of the slice: x: 4, y: 4, z: 1, core: 2. Of those that a mesh axis runs over, the one named last changes fastest.
The devices are a block of a 4x4x8 slice.
Arguments:
- hidden: bfloat16 [16, 18432], P('dp')
- ln_gain: bfloat16 [18432], replicated
- ln_bias: bfloat16 [18432], replicated
- w_q: bfloat16 [18432, 18432], P(None, 'tp')
- w_k: bfloat16 [18432, 1536], P(None, 'tp')
- w_v: bfloat16 [18432, 1536], P(None, 'tp')
- w_o: bfloat16 [18432, 18432], P('tp')
- k_cache: bfloat16 [16, 1024, 8, 192], P('dp', 'sp', 'tp')
- v_cache: bfloat16 [16, 1024, 8, 192], P('dp', 'sp', 'tp')
- lengths: int32 [16], P('dp')
Outputs:
- output 1: bfloat16 [16, 18432], P('dp')
- output 2: bfloat16 [16, 8, 192], P('dp', 'tp')
- output 3: bfloat16 [16, 8, 192], P('dp', 'tp')
All inputs are finite; a program needn't handle non-finite values.
Results may differ from the reference program's by a relative error of at most 0.00424821.
Values sent between devices are 32-bit elements.
A program may use at most 768 MiB of HBM per device.

```python
import jax
import jax.numpy as jnp
from jax import lax

D_MODEL = 18432
Q_HEADS = 96
KV_HEADS = 8
HEAD_DIM = 192
BATCH_ROWS = 16
SEQ_LEN = 1024
GROUP_SIZE = Q_HEADS // KV_HEADS
ROT_DIM = HEAD_DIM // 2


def norm_one_plus(hidden, ln_gain, ln_bias):
    wide = hidden.astype(jnp.float32)
    row_mean = jnp.mean(wide, axis=-1, keepdims=True)
    centred = wide - row_mean
    row_var = jnp.mean(centred * centred, axis=-1, keepdims=True)
    scaled = centred * lax.rsqrt(row_var + 1e-5)
    return (scaled * (1.0 + ln_gain.astype(jnp.float32)) + ln_bias.astype(jnp.float32)).astype(jnp.bfloat16)


def rotate_first(head_vecs, rot_pos):
    half_rot = ROT_DIM // 2
    inv_freq = 10000.0 ** (-2.0 * jnp.arange(half_rot, dtype=jnp.float32) / ROT_DIM)
    rot_angle = rot_pos.astype(jnp.float32)[..., None] * inv_freq
    cos_part = jnp.cos(rot_angle)
    sin_part = jnp.sin(rot_angle)
    lead_part = head_vecs[..., :half_rot]
    tail_part = head_vecs[..., half_rot:ROT_DIM]
    return jnp.concatenate([lead_part * cos_part - tail_part * sin_part, tail_part * cos_part + lead_part * sin_part, head_vecs[..., ROT_DIM:]], axis=-1)


def setup_inputs(seed: int = 0, part: int = 0) -> dict:
    shared_keys = jax.random.split(jax.random.key(seed), 6)
    part_keys = jax.random.split(jax.random.fold_in(jax.random.key(seed), part), 6)
    q_width = Q_HEADS * HEAD_DIM
    kv_width = KV_HEADS * HEAD_DIM
    seg_count = 16
    seg_len = SEQ_LEN // seg_count
    hidden = jax.random.normal(part_keys[0], (BATCH_ROWS, D_MODEL), jnp.float32)
    ln_gain = 0.5 * jax.random.normal(shared_keys[0], (D_MODEL,), jnp.float32)
    ln_bias = 0.5 * jax.random.normal(shared_keys[1], (D_MODEL,), jnp.float32)
    w_q = jax.random.normal(shared_keys[2], (D_MODEL, q_width), jnp.float32) * D_MODEL ** -0.5
    w_k = jax.random.normal(shared_keys[3], (D_MODEL, kv_width), jnp.float32) * D_MODEL ** -0.5
    w_v = jax.random.normal(shared_keys[4], (D_MODEL, kv_width), jnp.float32) * D_MODEL ** -0.5
    w_o = jax.random.normal(shared_keys[5], (q_width, D_MODEL), jnp.float32) * q_width ** -0.5
    seg_shape = (BATCH_ROWS, seg_count, 1, KV_HEADS, HEAD_DIM)
    full_shape = (BATCH_ROWS, seg_count, seg_len, KV_HEADS, HEAD_DIM)
    cache_shape = (BATCH_ROWS, SEQ_LEN, KV_HEADS, HEAD_DIM)
    k_cache = (jax.random.normal(part_keys[1], seg_shape, jnp.float32) + jax.random.normal(part_keys[2], full_shape, jnp.float32)).reshape(cache_shape)
    v_cache = (1.5 * jax.random.normal(part_keys[3], seg_shape, jnp.float32) + 0.5 * jax.random.normal(part_keys[4], full_shape, jnp.float32)).reshape(cache_shape)
    lengths = jax.random.randint(part_keys[5], (BATCH_ROWS,), SEQ_LEN // 8, SEQ_LEN, dtype=jnp.int32)
    lengths = lengths.at[0].set(SEQ_LEN - 1).at[BATCH_ROWS - 1].set(SEQ_LEN // 8)
    return {'hidden': hidden.astype(jnp.bfloat16), 'ln_gain': ln_gain.astype(jnp.bfloat16), 'ln_bias': ln_bias.astype(jnp.bfloat16), 'w_q': w_q.astype(jnp.bfloat16), 'w_k': w_k.astype(jnp.bfloat16), 'w_v': w_v.astype(jnp.bfloat16), 'w_o': w_o.astype(jnp.bfloat16), 'k_cache': k_cache.astype(jnp.bfloat16), 'v_cache': v_cache.astype(jnp.bfloat16), 'lengths': lengths}


def reference(hidden, ln_gain, ln_bias, w_q, w_k, w_v, w_o, k_cache, v_cache, lengths):
    normed = norm_one_plus(hidden, ln_gain, ln_bias)
    q_proj = jnp.dot(normed, w_q, preferred_element_type=jnp.float32).reshape(BATCH_ROWS, KV_HEADS, GROUP_SIZE, HEAD_DIM)
    queries = rotate_first(q_proj, lengths[:, None, None]).astype(jnp.bfloat16)
    k_proj = jnp.dot(normed, w_k, preferred_element_type=jnp.float32).reshape(BATCH_ROWS, KV_HEADS, HEAD_DIM)
    k_new = rotate_first(k_proj, lengths[:, None]).astype(jnp.bfloat16)
    v_new = jnp.dot(normed, w_v, preferred_element_type=jnp.float32).astype(jnp.bfloat16).reshape(BATCH_ROWS, KV_HEADS, HEAD_DIM)
    score_scale = HEAD_DIM ** -0.5
    positions = jnp.arange(SEQ_LEN)

    def one_sequence(row_args):
        q_row, k_row, v_row, k_self, v_self, length = row_args
        q_wide = q_row.astype(jnp.float32)
        scores = jnp.einsum('kgd,skd->kgs', q_wide, k_row.astype(jnp.float32)) * score_scale
        scores = jnp.where(positions < length, scores, -jnp.inf)
        self_score = jnp.einsum('kgd,kd->kg', q_wide, k_self.astype(jnp.float32)) * score_scale
        row_max = jnp.maximum(jnp.max(scores, axis=-1), self_score)
        weights = jnp.exp(scores - row_max[..., None])
        self_weight = jnp.exp(self_score - row_max)
        weight_sum = jnp.sum(weights, axis=-1) + self_weight
        narrow_w = weights.astype(jnp.bfloat16).astype(jnp.float32)
        weighted = jnp.einsum('kgs,skd->kgd', narrow_w, v_row.astype(jnp.float32))
        weighted = weighted + self_weight[..., None] * v_self.astype(jnp.float32)[:, None, :]
        return (weighted / weight_sum[..., None]).astype(jnp.bfloat16)

    context = lax.map(one_sequence, (queries, k_cache, v_cache, k_new, v_new, lengths))
    attn_out = jnp.dot(context.reshape(BATCH_ROWS, Q_HEADS * HEAD_DIM), w_o, preferred_element_type=jnp.float32)
    out = (hidden.astype(jnp.float32) + attn_out).astype(jnp.bfloat16)
    return (out, k_new, v_new)
```

```python
import functools

import jax
import jax.numpy as jnp
from jax import lax
from jax.experimental import pallas as pl
from jax.experimental.pallas import tpu as pltpu
from jax.sharding import PartitionSpec as P

F32 = jnp.float32
BF16 = jnp.bfloat16
MESH_ID = pl.DeviceIdType.MESH


def dot(a, b):
    return jnp.dot(a, b, preferred_element_type=F32)


def dot_t(a, b):
    return lax.dot_general(a, b, (((1,), (1,)), ((), ())), preferred_element_type=F32)


def rope(u, cos_t, sin_lo, sin_hi, half):
    width = u.shape[1]
    ahead = pltpu.roll(u, width - half, 1)
    behind = pltpu.roll(u, half, 1)
    return u * cos_t + ahead * sin_lo + behind * sin_hi


def kernel(cfg, hidden, gain, bias, w_q, w_k, w_v, w_o, k_t, v_t, lens, out, kv_out,
           hid_v, gb_raw, gb_f, h_v, len_s, wq_v, wkv_v, wo_v, kc_v, vc_v, k_snd, v_snd, k_rcv, v_rcv,
           qp, q_in, q_all, qh, kvp, kv_in, kv_all, kvn, score, ob, o_in, ctx_own, ctx_in, acc, rs_in,
           sem_small, sem_cache, sem_wq, sem_wkv, sem_wo,
           s_cx, r_cx, s_qd, r_qd, s_qg, r_qg, s_kd, r_kd, s_kg, r_kg, s_ke, r_ke,
           s_cr, r_cr, s_cg, r_cg, s_cf, r_cf, s_rs, r_rs, s_og, r_og, s_of, r_of):
    XN, TN, HD, G, KC, scale = cfg
    B, D = hidden.shape
    BH = B // 2
    SL = k_t.shape[3]
    KVN = k_t.shape[1]
    QW = w_q.shape[1] // XN
    KH = D // 2
    KVR = KH // (XN // 2)
    HB = QW // HD
    OW = D // (2 * XN)
    PW = OW // 2
    rot = HD // 2
    half = rot // 2
    strip = 2 * HD
    RB = HB * BH

    t = lax.axis_index('tp')
    s = lax.axis_index('sp')
    x = s // 2
    c = s % 2
    other = s + 1 - 2 * c
    xs = [(x + d) % XN for d in range(XN)]
    ts = [(t + d) % TN for d in range(TN)]
    partner = {'sp': other}

    def xpeer(d):
        return {'sp': 2 * xs[d] + c}

    def remote(src, dst, ss, rs, dev):
        return pltpu.make_async_remote_copy(src_ref=src, dst_ref=dst, send_sem=ss, recv_sem=rs, device_id=dev, device_id_type=MESH_ID)

    mine = pl.ds(pl.multiple_of(c * BH, BH), BH)
    theirs = pl.ds(pl.multiple_of((1 - c) * BH, BH), BH)

    c_hid = pltpu.make_async_copy(hidden, hid_v, sem_small.at[0])
    c_gain = pltpu.make_async_copy(gain, gb_raw.at[0], sem_small.at[1])
    c_bias = pltpu.make_async_copy(bias, gb_raw.at[1], sem_small.at[2])
    c_len = pltpu.make_async_copy(lens, len_s, sem_small.at[3])
    for cp in (c_hid, c_gain, c_bias, c_len):
        cp.start()
    c_cache = [pltpu.make_async_copy(k_t.at[theirs], kc_v.at[theirs], sem_cache.at[0]),
               pltpu.make_async_copy(v_t.at[theirs], vc_v.at[theirs], sem_cache.at[1]),
               pltpu.make_async_copy(k_t.at[mine], kc_v.at[mine], sem_cache.at[2]),
               pltpu.make_async_copy(v_t.at[mine], vc_v.at[mine], sem_cache.at[3])]
    qcol = pl.ds(pl.multiple_of(x * QW, 128), QW)
    NQ = KH // KC

    def wq_copy(i):
        return pltpu.make_async_copy(w_q.at[pl.ds(pl.multiple_of(c * KH + i * KC, KC), KC), qcol], wq_v.at[i], sem_wq.at[i])

    for i in range(2):
        wq_copy(i).start()
    c_cache[0].start()
    c_cache[1].start()
    for i in range(2, NQ):
        wq_copy(i).start()
    c_cache[2].start()
    c_cache[3].start()
    kvrow = pl.ds(pl.multiple_of(c * KH + (x % (XN // 2)) * KVR, KVR), KVR)
    c_wk = pltpu.make_async_copy(w_k.at[kvrow, :], wkv_v, sem_wkv.at[0])
    c_wv = pltpu.make_async_copy(w_v.at[kvrow, :], wkv_v, sem_wkv.at[0])

    @pl.when(x < XN // 2)
    def _():
        c_wk.start()

    @pl.when(x >= XN // 2)
    def _():
        c_wv.start()

    ocol = pl.ds(pl.multiple_of(s * OW, 128), OW)

    def wo_copy(d):
        return pltpu.make_async_copy(w_o.at[pl.ds(pl.multiple_of(xs[d] * QW, QW), QW), ocol], wo_v.at[d], sem_wo.at[d])

    for d in (0, 1, XN - 1) + tuple(range(2, XN - 1)):
        wo_copy(d).start()

    barrier = pltpu.get_barrier_semaphore()
    pl.semaphore_signal(barrier, inc=1, device_id=partner, device_id_type=MESH_ID)
    for dx in range(XN):
        for dt in range(TN):
            if dx or dt:
                pl.semaphore_signal(barrier, inc=1, device_id={'tp': ts[dt], 'sp': 2 * xs[dx] + c}, device_id_type=MESH_ID)

    c_hid.wait()
    nt = D // 128
    UN = 8

    def sum_step(i, a):
        for u in range(UN):
            a = a + hid_v[:, pl.ds(pl.multiple_of((i * UN + u) * 128, 128), 128)].astype(F32)
        return a

    tot = lax.fori_loop(0, nt // UN, sum_step, jnp.zeros((B, 128), F32))
    mean = jnp.sum(tot, axis=1, keepdims=True) / D

    def var_step(i, a):
        for u in range(UN):
            v = hid_v[:, pl.ds(pl.multiple_of((i * UN + u) * 128, 128), 128)].astype(F32) - mean
            a = a + v * v
        return a

    sq = lax.fori_loop(0, nt // UN, var_step, jnp.zeros((B, 128), F32))
    rstd = lax.rsqrt(jnp.sum(sq, axis=1, keepdims=True) / D + 1e-5)
    c_gain.wait()
    c_bias.wait()
    gb_f[0] = 1.0 + gb_raw[0].astype(F32)
    gb_f[1] = gb_raw[1].astype(F32)

    def norm_step(i, _):
        for u in range(UN):
            j = i * UN + u
            col = c * (nt // 2) + j
            v = hid_v[:, pl.ds(pl.multiple_of(col * 128, 128), 128)].astype(F32)
            v = (v - mean) * rstd * gb_f[0, pl.ds(col, 1), :] + gb_f[1, pl.ds(col, 1), :]
            h_v[:, pl.ds(pl.multiple_of(j * 128, 128), 128)] = v.astype(BF16)
        return 0

    lax.fori_loop(0, nt // 2 // UN, norm_step, 0)

    c_len.wait()
    row = lax.broadcasted_iota(jnp.int32, (BH, strip), 0)
    lane = lax.broadcasted_iota(jnp.int32, (BH, strip), 1)
    pos = jnp.zeros((BH, strip), F32)
    for r in range(BH):
        pos = jnp.where(row == r, len_s[c * BH + r].astype(F32), pos)
    hl = jnp.where(lane >= HD, lane - HD, lane)
    il = jnp.where(hl >= half, hl - half, hl)
    freq = jnp.exp(il.astype(F32) * (-2.0 / rot * 9.210340371976184))
    ang = jnp.where(hl < rot, pos * freq, 0.0)
    cos_t = jnp.cos(ang)
    sin_t = jnp.sin(ang)
    sin_lo = jnp.where(hl < half, -sin_t, 0.0)
    sin_hi = jnp.where(hl >= half, sin_t, 0.0)

    pl.semaphore_wait(barrier, XN * TN)

    def q_step(i, a):
        wq_copy(i).wait()
        return a + dot(h_v[:, pl.ds(pl.multiple_of(i * KC, KC), KC)], wq_v[i])

    NB = 4
    a = lax.fori_loop(0, NB, q_step, jnp.zeros((B, QW), F32))

    c_cache[0].wait()
    c_cache[1].wait()

    def widen(b, _):
        k_snd[b] = kc_v[(1 - c) * BH + b].astype(F32)
        v_snd[b] = vc_v[(1 - c) * BH + b].astype(F32)
        return 0

    lax.fori_loop(0, BH, widen, 0)
    xk = remote(k_snd, k_rcv, s_cx.at[0], r_cx.at[0], partner)
    xv = remote(v_snd, v_rcv, s_cx.at[1], r_cx.at[1], partner)
    xk.start()
    xv.start()

    qp[...] = lax.fori_loop(NB, NQ, q_step, a)
    xq = remote(qp.at[theirs, :], q_in, s_qd.at[0], r_qd.at[0], partner)
    xq.start()

    @pl.when(x < XN // 2)
    def _():
        c_wk.wait()

    @pl.when(x >= XN // 2)
    def _():
        c_wv.wait()

    xq.wait()
    qb = qp[mine, :] + q_in[...]
    for i in range(QW // strip):
        sl = slice(i * strip, (i + 1) * strip)
        q_all[x, :, sl] = rope(qb[:, sl], cos_t, sin_lo, sin_hi, half).astype(BF16).astype(F32)
    qg = []
    for d in range(1, XN):
        cp = remote(q_all.at[x], q_all.at[x], s_qg.at[d], r_qg.at[x], xpeer(d))
        cp.start()
        qg.append(cp)

    kvp[...] = dot(h_v[:, pl.ds(pl.multiple_of((x % (XN // 2)) * KVR, KVR), KVR)], wkv_v[...])
    xkd = remote(kvp.at[theirs, :], kv_in, s_kd.at[0], r_kd.at[0], partner)
    xkd.start()
    xkd.wait()
    kv_all[x] = kvp[mine, :] + kv_in[...]
    kg = []
    for d in range(1, XN):
        cp = remote(kv_all.at[x], kv_all.at[x], s_kg.at[d], r_kg.at[x], xpeer(d))
        cp.start()
        kg.append(cp)

    for d in range(XN):
        if d:
            remote(q_all.at[x], q_all.at[xs[d]], s_qg.at[d], r_qg.at[xs[d]], xpeer(d)).wait_recv()
    for blk in range(XN):
        for j in range(HB):
            h = blk * HB + j
            v = q_all[blk, :, j * HD:(j + 1) * HD]
            qh[0, h * BH:(h + 1) * BH, :] = v[:, 0:128]
            qh[1, h * BH:(h + 1) * BH, 0:HD - 128] = v[:, 128:HD]

    c_cache[2].wait()
    c_cache[3].wait()
    xk.wait()
    xv.wait()
    lane2 = lax.broadcasted_iota(jnp.int32, (G, 2 * SL), 1)
    p_here = jnp.where(lane2 < SL, s * SL + lane2, other * SL + lane2 - SL)
    for b in range(BH):
        for kv in range(KVN):
            rows = pl.ds(kv * G * BH + b, G, stride=BH)
            q = jnp.concatenate([qh[0, rows, :], qh[1, rows, :]], axis=1)[:, 0:HD].astype(BF16)
            s0 = dot(q, kc_v[c * BH + b, kv])
            s1 = dot(q, k_rcv[b, kv].astype(BF16))
            score[b, kv] = jnp.concatenate([s0, s1], axis=1)
    neg = -jnp.inf
    tail_lane = lax.broadcasted_iota(jnp.int32, (G, 128), 1)
    for b in range(BH):
        n = len_s[c * BH + b]
        for kv in range(KVN):
            sc = jnp.where(p_here < n, score[b, kv] * scale, neg)
            m = jnp.max(sc, axis=1, keepdims=True)
            ms = jnp.where(m == neg, 0.0, m)
            w = jnp.exp(sc - ms)
            l = jnp.sum(w, axis=1, keepdims=True)
            wb = w.astype(BF16)
            pv = dot_t(wb[:, 0:SL], vc_v[c * BH + b, kv]) + dot_t(wb[:, SL:], v_rcv[b, kv].astype(BF16))
            tail = jnp.concatenate([pv[:, 128:HD], jnp.zeros((G, 256 - HD), F32)], axis=1)
            tail = jnp.where(tail_lane == HD - 128, m, jnp.where(tail_lane == HD - 127, l, tail))
            rows = pl.ds(kv * G * BH + b, G, stride=BH)
            ob[0, rows, :] = pv[:, 0:128]
            ob[1, rows, :] = tail

    cr = []
    for d in range(1, XN):
        cp = remote(ob.at[:, pl.ds(pl.multiple_of(xs[d] * RB, RB), RB), :], o_in.at[x], s_cr.at[d], r_cr.at[x], xpeer(d))
        cp.start()
        cr.append(cp)

    for d in range(1, XN):
        remote(kv_all.at[x], kv_all.at[xs[d]], s_kg.at[d], r_kg.at[xs[d]], xpeer(d)).wait_recv()
    kn = kv_all[0]
    vn = kv_all[XN // 2]
    for i in range(1, XN // 2):
        kn = kn + kv_all[i]
        vn = vn + kv_all[XN // 2 + i]
    kn = rope(kn, cos_t, sin_lo, sin_hi, half).astype(BF16).astype(F32)
    vn = vn.astype(BF16).astype(F32)
    kvn[:, 0:strip] = kn
    kvn[:, strip:2 * strip] = vn
    kv_out[mine, :] = kvn[...]
    xe = remote(kvn, kv_out.at[mine, :], s_ke.at[0], r_ke.at[0], partner)
    xe.start()
    second = x >= XN // 2
    kh = jnp.where(second, kn[:, HD:], kn[:, 0:HD])
    vh = jnp.where(second, vn[:, HD:], vn[:, 0:HD])

    own = pl.ds(pl.multiple_of(x * RB, RB), RB)
    q_own = jnp.concatenate([qh[0, own, :], qh[1, own, :]], axis=1)[:, 0:HD]
    k_rep = jnp.concatenate([kh] * HB, axis=0)
    v_rep = jnp.concatenate([vh] * HB, axis=0)
    self_s = jnp.sum(q_own * k_rep, axis=1, keepdims=True) * scale
    for d in range(1, XN):
        remote(ob.at[:, own, :], o_in.at[xs[d]], s_cr.at[d], r_cr.at[xs[d]], xpeer(d)).wait_recv()
    o_in[x] = ob[:, own, :]
    parts = [jnp.concatenate([o_in[i, 0], o_in[i, 1]], axis=1) for i in range(XN)]
    ms = [p[:, HD:HD + 1] for p in parts]
    ls = [p[:, HD + 1:HD + 2] for p in parts]
    top = self_s
    for m in ms:
        top = jnp.maximum(top, m)
    f_self = jnp.exp(self_s - top)
    num = f_self * v_rep
    den = f_self
    for p, m, l in zip(parts, ms, ls):
        f = jnp.exp(m - top)
        num = num + f * p[:, 0:HD]
        den = den + f * l
    ctx = (num / den).astype(BF16).astype(F32)
    for j in range(HB):
        ctx_own[:, j * HD:(j + 1) * HD] = ctx[j * BH:(j + 1) * BH, :]

    cg = []
    cf = []
    ctx_in[x, mine, :] = ctx_own[...]
    cp = remote(ctx_own, ctx_in.at[x, mine, :], s_cf.at[0], r_cf.at[x], partner)
    cp.start()
    cf.append(cp)
    order = [1, XN - 1] + list(range(2, XN - 1))
    for d in order:
        cp = remote(ctx_own, ctx_in.at[x, mine, :], s_cg.at[d], r_cg.at[x], xpeer(d))
        cp.start()
        cg.append(cp)

    NW = 768
    for step, d in enumerate([0] + order):
        blk = xs[d]
        if d:
            remote(ctx_own, ctx_in.at[blk, mine, :], s_cg.at[d], r_cg.at[blk], xpeer(d)).wait_recv()
            cp = remote(ctx_in.at[blk, mine, :], ctx_in.at[blk, mine, :], s_cf.at[d], r_cf.at[blk], partner)
            cp.start()
            cf.append(cp)
        remote(ctx_own, ctx_in.at[blk, theirs, :], s_cf.at[d], r_cf.at[blk], partner).wait_recv()
        wo_copy(d).wait()
        lhs = ctx_in[blk].astype(BF16)
        for n in range(OW // NW):
            cs = slice(n * NW, (n + 1) * NW)
            r = dot(lhs, wo_v[d, :, cs])
            acc[:, cs] = r if step == 0 else acc[:, cs] + r

    def part(p):
        return (pl.ds(pl.multiple_of((p % 2) * BH, BH), BH), pl.ds(pl.multiple_of((p // 2) * PW, 128), PW))

    rsl = []
    for d in range(1, TN):
        rows, cols = part(ts[d])
        cp = remote(acc.at[rows, cols], rs_in.at[t], s_rs.at[d], r_rs.at[t], {'tp': ts[d]})
        cp.start()
        rsl.append(cp)
    rows, cols = part(t)
    for d in range(1, TN):
        remote(acc.at[rows, cols], rs_in.at[ts[d]], s_rs.at[d], r_rs.at[ts[d]], {'tp': ts[d]}).wait_recv()
    rs_in[t] = acc[rows, cols]
    tot = rs_in[0]
    for i in range(1, TN):
        tot = tot + rs_in[i]

    def place(sv, p):
        return out.at[pl.ds(pl.multiple_of((p % 2) * BH, BH), BH), pl.ds(pl.multiple_of(sv * OW + (p // 2) * PW, 128), PW)]

    place(s, t)[...] = tot
    og = []
    for dx in range(XN):
        for dt in range(TN):
            if dx or dt:
                cp = remote(place(s, t), place(s, t), s_og.at[dx * TN + dt], r_og.at[x * TN + t], {'tp': ts[dt], 'sp': 2 * xs[dx] + c})
                cp.start()
                og.append(cp)
    of = []
    for dx in range(XN):
        for dt in range(TN):
            src = place(2 * xs[dx] + c, ts[dt])
            if dx or dt:
                remote(src, src, s_og.at[dx * TN + dt], r_og.at[xs[dx] * TN + ts[dt]], partner).wait_recv()
            cp = remote(src, src, s_of.at[dx * TN + dt], r_of.at[xs[dx] * TN + ts[dt]], partner)
            cp.start()
            of.append(cp)
    for dx in range(XN):
        for dt in range(TN):
            src = place(2 * xs[dx] + 1 - c, ts[dt])
            remote(src, src, s_of.at[dx * TN + dt], r_of.at[xs[dx] * TN + ts[dt]], partner).wait_recv()
    xe_in = remote(kvn, kv_out.at[theirs, :], s_ke.at[0], r_ke.at[0], partner)
    xe_in.wait_recv()
    for cp in qg + kg + cr + [xe] + cg + cf + rsl + og + of:
        cp.wait_send()


def solution(mesh):
    TN = mesh.shape['tp']
    SN = mesh.shape['sp']
    XN = SN // 2

    def local_step(hidden, ln_gain, ln_bias, w_q, w_k, w_v, w_o, k_cache, v_cache, lengths):
        B, D = hidden.shape
        _, SL, KVN, HD = k_cache.shape
        G = w_q.shape[1] // (HD * KVN)
        BH = B // 2
        QW = w_q.shape[1] // XN
        KH = D // 2
        KC = 1024
        NQ = KH // KC
        KVR = KH // (XN // 2)
        HB = QW // HD
        OW = D // SN
        PW = OW // 2
        KW = KVN * HD
        assert w_k.shape[1] == KW and KH % KC == 0 and TN == 4 and XN % 2 == 0 and KVN == 2
        k_t = jnp.transpose(k_cache, (0, 2, 3, 1))
        v_t = jnp.transpose(v_cache, (0, 2, 3, 1))
        gain = ln_gain.reshape(D // 128, 128)
        bias = ln_bias.reshape(D // 128, 128)
        V = pltpu.VMEM
        dma = pltpu.SemaphoreType.DMA
        scratch = [
            V((B, D), BF16), V((2, D // 128, 128), BF16), V((2, D // 128, 128), F32), V((B, KH), BF16), pltpu.SMEM((B,), jnp.int32),
            V((NQ, KC, QW), BF16), V((KVR, KW), BF16), V((XN, QW, OW), BF16),
            V((B, KVN, HD, SL), BF16), V((B, KVN, HD, SL), BF16),
            V((BH, KVN, HD, SL), F32), V((BH, KVN, HD, SL), F32), V((BH, KVN, HD, SL), F32), V((BH, KVN, HD, SL), F32),
            V((B, QW), F32), V((BH, QW), F32), V((XN, BH, QW), F32), V((2, XN * HB * BH, 128), F32),
            V((B, KW), F32), V((BH, KW), F32), V((XN, BH, KW), F32), V((BH, 2 * KW), F32),
            V((BH, KVN, G, 2 * SL), F32), V((2, XN * HB * BH, 128), F32), V((XN, 2, HB * BH, 128), F32),
            V((BH, QW), F32), V((XN, B, QW), F32), V((B, OW), F32), V((TN, BH, PW), F32),
            dma((4,)), dma((4,)), dma((NQ,)), dma((1,)), dma((XN,)),
            dma((2,)), dma((2,)), dma((1,)), dma((1,)), dma((XN,)), dma((XN,)), dma((1,)), dma((1,)), dma((XN,)), dma((XN,)), dma((1,)), dma((1,)),
            dma((XN,)), dma((XN,)), dma((XN,)), dma((XN,)), dma((XN,)), dma((XN,)), dma((TN,)), dma((TN,)),
            dma((XN * TN,)), dma((XN * TN,)), dma((XN * TN,)), dma((XN * TN,)),
        ]
        cfg = (XN, TN, HD, G, KC, HD ** -0.5)
        summed, kv_new = pl.pallas_call(
            functools.partial(kernel, cfg),
            out_shape=(jax.ShapeDtypeStruct((B, D), F32), jax.ShapeDtypeStruct((B, 2 * KW), F32)),
            in_specs=[pl.BlockSpec(memory_space=pl.ANY)] * 10,
            out_specs=(pl.BlockSpec(memory_space=pltpu.VMEM), pl.BlockSpec(memory_space=pltpu.VMEM)),
            scratch_shapes=scratch,
            compiler_params=pltpu.CompilerParams(collective_id=0, has_side_effects=True, vmem_limit_bytes=67043328),
            name='decode_step',
        )(hidden, gain, bias, w_q, w_k, w_v, w_o, k_t, v_t, lengths)
        out = (hidden.astype(F32) + summed).astype(BF16)
        k_new = kv_new[:, :KW].astype(BF16).reshape(B, KVN, HD)
        v_new = kv_new[:, KW:].astype(BF16).reshape(B, KVN, HD)
        return out, k_new, v_new

    row_spec = P('dp', None)
    cache_spec = P('dp', 'sp', 'tp', None)
    head_spec = P('dp', 'tp', None)
    return jax.shard_map(local_step, mesh=mesh, in_specs=(row_spec, P(None), P(None), P(None, 'tp'), P(None, 'tp'), P(None, 'tp'), P('tp', None), cache_spec, cache_spec, P('dp')), out_specs=(row_spec, head_spec, head_spec), check_vma=False)
```

```python
import functools

import jax
import jax.numpy as jnp
from jax import lax
from jax.experimental import pallas as pl
from jax.experimental.pallas import tpu as pltpu
from jax.sharding import PartitionSpec as P

F32 = jnp.float32
BF16 = jnp.bfloat16
MESH_ID = pl.DeviceIdType.MESH


def dot(a, b):
    return jnp.dot(a, b, preferred_element_type=F32)


def dot_t(a, b):
    return lax.dot_general(a, b, (((1,), (1,)), ((), ())), preferred_element_type=F32)


def rope(u, cos_t, sin_lo, sin_hi, half):
    width = u.shape[1]
    ahead = pltpu.roll(u, width - half, 1)
    behind = pltpu.roll(u, half, 1)
    return u * cos_t + ahead * sin_lo + behind * sin_hi


def kernel(cfg, hidden, gain, bias, w_q, w_k, w_v, w_o, k_t, v_t, lens, out, k_out, v_out,
           hid_v, gb_raw, gb_f, h_v, len_s, wq_v, wkv_v, wo_v, kc_v, vc_v, k_snd, v_snd, k_rcv, v_rcv,
           og_v, ob_v, kv_rcv, qp, q_in, q_all, qh, kvp, kv_in, kv_all, kvn, score, ob, o_in, ctx_own, ctx_all, part, p1_in, p2_in,
           sem_small, sem_cache, sem_wq, sem_wkv, sem_wo, sem_out,
           s_cx, r_cx, s_qd, r_qd, s_qg, r_qg, s_kd, r_kd, s_kg, r_kg, s_ke, r_ke,
           s_cr, r_cr, s_cf, r_cf, s_p1, r_p1, s_p2, r_p2, s_ag, r_ag, s_of, r_of):
    XN, TN, HD, G, KC, scale = cfg
    B, D = hidden.shape
    BH = B // 2
    SL = k_t.shape[3]
    KVN = k_t.shape[1]
    QW = w_q.shape[1] // XN
    KH = D // 2
    KVR = KH // (XN // 2)
    HB = QW // HD
    OW = D // (2 * XN)
    PW = OW // 2
    NP = 4
    rot = HD // 2
    half = rot // 2
    strip = 2 * HD
    RB = HB * BH

    t = lax.axis_index('tp')
    s = lax.axis_index('sp')
    x = s // 2
    c = s % 2
    other = s + 1 - 2 * c
    xs = [(x + d) % XN for d in range(XN)]
    ts = [(t + d) % TN for d in range(TN)]
    partner = {'sp': other}

    def xpeer(d):
        return {'sp': 2 * xs[d] + c}

    def remote(src, dst, ss, rs, dev):
        return pltpu.make_async_remote_copy(src_ref=src, dst_ref=dst, send_sem=ss, recv_sem=rs, device_id=dev, device_id_type=MESH_ID)

    mine = pl.ds(pl.multiple_of(c * BH, BH), BH)
    theirs = pl.ds(pl.multiple_of((1 - c) * BH, BH), BH)

    c_hid = pltpu.make_async_copy(hidden, hid_v, sem_small.at[0])
    c_gain = pltpu.make_async_copy(gain, gb_raw.at[0], sem_small.at[1])
    c_bias = pltpu.make_async_copy(bias, gb_raw.at[1], sem_small.at[2])
    c_len = pltpu.make_async_copy(lens, len_s, sem_small.at[3])
    for cp in (c_hid, c_gain, c_bias, c_len):
        cp.start()
    c_cache = [pltpu.make_async_copy(k_t.at[theirs], kc_v.at[theirs], sem_cache.at[0]),
               pltpu.make_async_copy(v_t.at[theirs], vc_v.at[theirs], sem_cache.at[1]),
               pltpu.make_async_copy(k_t.at[mine], kc_v.at[mine], sem_cache.at[2]),
               pltpu.make_async_copy(v_t.at[mine], vc_v.at[mine], sem_cache.at[3])]
    qcol = pl.ds(pl.multiple_of(x * QW, 128), QW)
    NQ = KH // KC

    def wq_copy(i):
        return pltpu.make_async_copy(w_q.at[pl.ds(pl.multiple_of(c * KH + i * KC, KC), KC), qcol], wq_v.at[i], sem_wq.at[i])

    c_cache[0].start()
    c_cache[1].start()
    wq_copy(0).start()
    wq_copy(1).start()
    kvrow = pl.ds(pl.multiple_of(c * KH + (x % (XN // 2)) * KVR, KVR), KVR)
    c_wk = pltpu.make_async_copy(w_k.at[kvrow, :], wkv_v, sem_wkv.at[0])
    c_wv = pltpu.make_async_copy(w_v.at[kvrow, :], wkv_v, sem_wkv.at[0])

    def start_wkv():
        @pl.when(x < XN // 2)
        def _():
            c_wk.start()

        @pl.when(x >= XN // 2)
        def _():
            c_wv.start()

    k1 = x * (1 - c) + t * c
    k2 = x * c + t * (1 - c)
    k1s = [(k1 + d) % XN for d in range(XN)]
    k2s = [(k2 + d) % XN for d in range(XN)]

    def along1(d):
        return {'tp': (t + c * d) % TN, 'sp': 2 * ((x + (1 - c) * d) % XN) + c}

    def along2(d):
        return {'tp': (t + (1 - c) * d) % TN, 'sp': 2 * ((x + c * d) % XN) + c}

    def wo_copy(d):
        cols = pl.ds(pl.multiple_of(c * (D // 2) + k1s[d] * OW, 128), OW)
        return pltpu.make_async_copy(w_o.at[pl.ds(pl.multiple_of(x * QW, QW), QW), cols], wo_v.at[d], sem_wo.at[d])

    order = [1, XN - 1] + list(range(2, XN - 1))
    later = [functools.partial(lambda i: wq_copy(i).start(), i) for i in range(2, NQ)]
    later += [start_wkv, c_cache[2].start, c_cache[3].start]
    far_first = [2, 1, 3, 0]
    later += [functools.partial(lambda d: wo_copy(d).start(), d) for d in far_first]

    def issue(n):
        for _ in range(n):
            if later:
                later.pop(0)()

    barrier = pltpu.get_barrier_semaphore()
    pl.semaphore_signal(barrier, inc=1, device_id=partner, device_id_type=MESH_ID)
    for dx in range(XN):
        for dt in range(TN):
            if dx or dt:
                pl.semaphore_signal(barrier, inc=1, device_id={'tp': ts[dt], 'sp': 2 * xs[dx] + c}, device_id_type=MESH_ID)

    c_hid.wait()
    nt = D // 128
    UN = 8

    def sum_step(i, a):
        for u in range(UN):
            a = a + hid_v[:, pl.ds(pl.multiple_of((i * UN + u) * 128, 128), 128)].astype(F32)
        return a

    tot = lax.fori_loop(0, nt // UN, sum_step, jnp.zeros((B, 128), F32))
    mean = jnp.sum(tot, axis=1, keepdims=True) / D

    def var_step(i, a):
        for u in range(UN):
            v = hid_v[:, pl.ds(pl.multiple_of((i * UN + u) * 128, 128), 128)].astype(F32) - mean
            a = a + v * v
        return a

    sq = lax.fori_loop(0, nt // UN, var_step, jnp.zeros((B, 128), F32))
    issue(1)
    rstd = lax.rsqrt(jnp.sum(sq, axis=1, keepdims=True) / D + 1e-5)
    c_gain.wait()
    c_bias.wait()
    issue(1)
    gb_f[0] = 1.0 + gb_raw[0].astype(F32)
    gb_f[1] = gb_raw[1].astype(F32)

    def norm_step(i, _):
        for u in range(UN):
            j = i * UN + u
            col = c * (nt // 2) + j
            v = hid_v[:, pl.ds(pl.multiple_of(col * 128, 128), 128)].astype(F32)
            v = (v - mean) * rstd * gb_f[0, pl.ds(col, 1), :] + gb_f[1, pl.ds(col, 1), :]
            h_v[:, pl.ds(pl.multiple_of(j * 128, 128), 128)] = v.astype(BF16)
        return 0

    lax.fori_loop(0, nt // 2 // UN, norm_step, 0)

    c_len.wait()
    row = lax.broadcasted_iota(jnp.int32, (BH, strip), 0)
    lane = lax.broadcasted_iota(jnp.int32, (BH, strip), 1)
    pos = jnp.zeros((BH, strip), F32)
    for r in range(BH):
        pos = jnp.where(row == r, len_s[c * BH + r].astype(F32), pos)
    hl = jnp.where(lane >= HD, lane - HD, lane)
    il = jnp.where(hl >= half, hl - half, hl)
    freq = jnp.exp(il.astype(F32) * (-2.0 / rot * 9.210340371976184))
    ang = jnp.where(hl < rot, pos * freq, 0.0)
    cos_t = jnp.cos(ang)
    sin_t = jnp.sin(ang)
    sin_lo = jnp.where(hl < half, -sin_t, 0.0)
    sin_hi = jnp.where(hl >= half, sin_t, 0.0)

    pl.semaphore_wait(barrier, XN * TN)

    c_cache[0].wait()
    c_cache[1].wait()

    def widen(b, _):
        k_snd[b] = kc_v[(1 - c) * BH + b].astype(F32)
        v_snd[b] = vc_v[(1 - c) * BH + b].astype(F32)
        return 0

    lax.fori_loop(0, BH, widen, 0)
    xk = remote(k_snd, k_rcv, s_cx.at[0], r_cx.at[0], partner)
    xv = remote(v_snd, v_rcv, s_cx.at[1], r_cx.at[1], partner)
    xk.start()
    xv.start()

    a = None
    for i in range(NQ):
        wq_copy(i).wait()
        issue(1)
        r = dot(h_v[:, i * KC:(i + 1) * KC], wq_v[i])
        a = r if a is None else a + r
    issue(len(later))
    qp[...] = a
    xq = remote(qp.at[theirs, :], q_in, s_qd.at[0], r_qd.at[0], partner)
    xq.start()

    xq.wait()
    qb = qp[mine, :] + q_in[...]
    for i in range(QW // strip):
        sl = slice(i * strip, (i + 1) * strip)
        q_all[x, :, sl] = rope(qb[:, sl], cos_t, sin_lo, sin_hi, half).astype(BF16).astype(F32)
    qg = []
    for d in range(1, XN):
        cp = remote(q_all.at[x], q_all.at[x], s_qg.at[d], r_qg.at[x], xpeer(d))
        cp.start()
        qg.append(cp)

    @pl.when(x < XN // 2)
    def _():
        c_wk.wait()

    @pl.when(x >= XN // 2)
    def _():
        c_wv.wait()

    kvp[...] = dot(h_v[:, pl.ds(pl.multiple_of((x % (XN // 2)) * KVR, KVR), KVR)], wkv_v[...])
    xkd = remote(kvp.at[theirs, :], kv_in, s_kd.at[0], r_kd.at[0], partner)
    xkd.start()
    xkd.wait()
    kv_all[x] = kvp[mine, :] + kv_in[...]
    kg = []
    for d in range(1, XN):
        cp = remote(kv_all.at[x], kv_all.at[x], s_kg.at[d], r_kg.at[x], xpeer(d))
        cp.start()
        kg.append(cp)

    for d in range(XN):
        if d:
            remote(q_all.at[x], q_all.at[xs[d]], s_qg.at[d], r_qg.at[xs[d]], xpeer(d)).wait_recv()
    for blk in range(XN):
        for j in range(HB):
            h = blk * HB + j
            v = q_all[blk, :, j * HD:(j + 1) * HD]
            qh[0, h * BH:(h + 1) * BH, :] = v[:, 0:128]
            qh[1, h * BH:(h + 1) * BH, 0:HD - 128] = v[:, 128:HD]

    c_cache[2].wait()
    c_cache[3].wait()
    xk.wait()
    xv.wait()
    lane2 = lax.broadcasted_iota(jnp.int32, (G, 2 * SL), 1)
    p_here = jnp.where(lane2 < SL, s * SL + lane2, other * SL + lane2 - SL)
    for b in range(BH):
        for kv in range(KVN):
            rows = pl.ds(kv * G * BH + b, G, stride=BH)
            q = jnp.concatenate([qh[0, rows, :], qh[1, rows, :]], axis=1)[:, 0:HD].astype(BF16)
            s0 = dot(q, kc_v[c * BH + b, kv])
            s1 = dot(q, k_rcv[b, kv].astype(BF16))
            score[b, kv] = jnp.concatenate([s0, s1], axis=1)
    neg = -jnp.inf
    tail_lane = lax.broadcasted_iota(jnp.int32, (G, 128), 1)
    for b in range(BH):
        n = len_s[c * BH + b]
        for kv in range(KVN):
            sc = jnp.where(p_here < n, score[b, kv] * scale, neg)
            m = jnp.max(sc, axis=1, keepdims=True)
            ms = jnp.where(m == neg, 0.0, m)
            w = jnp.exp(sc - ms)
            l = jnp.sum(w, axis=1, keepdims=True)
            wb = w.astype(BF16)
            pv = dot_t(wb[:, 0:SL], vc_v[c * BH + b, kv]) + dot_t(wb[:, SL:], v_rcv[b, kv].astype(BF16))
            tail = jnp.concatenate([pv[:, 128:HD], jnp.zeros((G, 256 - HD), F32)], axis=1)
            tail = jnp.where(tail_lane == HD - 128, m, jnp.where(tail_lane == HD - 127, l, tail))
            rows = pl.ds(kv * G * BH + b, G, stride=BH)
            ob[0, rows, :] = pv[:, 0:128]
            ob[1, rows, :] = tail

    cr = []
    for d in range(1, XN):
        cp = remote(ob.at[:, pl.ds(pl.multiple_of(xs[d] * RB, RB), RB), :], o_in.at[x], s_cr.at[d], r_cr.at[x], xpeer(d))
        cp.start()
        cr.append(cp)

    for d in range(1, XN):
        remote(kv_all.at[x], kv_all.at[xs[d]], s_kg.at[d], r_kg.at[xs[d]], xpeer(d)).wait_recv()
    kn = kv_all[0]
    vn = kv_all[XN // 2]
    for i in range(1, XN // 2):
        kn = kn + kv_all[i]
        vn = vn + kv_all[XN // 2 + i]
    kn = rope(kn, cos_t, sin_lo, sin_hi, half).astype(BF16).astype(F32)
    vn = vn.astype(BF16).astype(F32)
    kvn[:, 0:strip] = kn
    kvn[:, strip:2 * strip] = vn
    kv_rcv[mine, :] = kvn[...]
    xe = remote(kvn, kv_rcv.at[mine, :], s_ke.at[0], r_ke.at[0], partner)
    xe.start()
    second = x >= XN // 2
    kh = jnp.where(second, kn[:, HD:], kn[:, 0:HD])
    vh = jnp.where(second, vn[:, HD:], vn[:, 0:HD])

    own = pl.ds(pl.multiple_of(x * RB, RB), RB)
    q_own = jnp.concatenate([qh[0, own, :], qh[1, own, :]], axis=1)[:, 0:HD]
    k_rep = jnp.concatenate([kh] * HB, axis=0)
    v_rep = jnp.concatenate([vh] * HB, axis=0)
    self_s = jnp.sum(q_own * k_rep, axis=1, keepdims=True) * scale
    for d in range(1, XN):
        remote(ob.at[:, own, :], o_in.at[xs[d]], s_cr.at[d], r_cr.at[xs[d]], xpeer(d)).wait_recv()
    o_in[x] = ob[:, own, :]
    parts = [jnp.concatenate([o_in[i, 0], o_in[i, 1]], axis=1) for i in range(XN)]
    ms = [p[:, HD:HD + 1] for p in parts]
    ls = [p[:, HD + 1:HD + 2] for p in parts]
    top = self_s
    for m in ms:
        top = jnp.maximum(top, m)
    f_self = jnp.exp(self_s - top)
    num = f_self * v_rep
    den = f_self
    for p, m, l in zip(parts, ms, ls):
        f = jnp.exp(m - top)
        num = num + f * p[:, 0:HD]
        den = den + f * l
    ctx = (num / den).astype(BF16).astype(F32)
    for j in range(HB):
        ctx_own[:, j * HD:(j + 1) * HD] = ctx[j * BH:(j + 1) * BH, :]

    ctx_all[mine, :] = ctx_own[...]
    cf = remote(ctx_own, ctx_all.at[mine, :], s_cf.at[0], r_cf.at[0], partner)
    cf.start()
    remote(ctx_own, ctx_all.at[theirs, :], s_cf.at[0], r_cf.at[0], partner).wait_recv()

    lhs = ctx_all[...].astype(BF16)
    sends = [xe, cf]

    def send(src, dst, ss, rs, dev):
        cp = remote(src, dst, ss, rs, dev)
        cp.start()
        sends.append(cp)

    for d in far_first:
        wo_copy(d).wait()
    for h in range(2):
        for d in far_first:
            r = dot(lhs, wo_v[d, :, h * PW:(h + 1) * PW])
            part[d, 2 * h] = r[0:BH]
            part[d, 2 * h + 1] = r[BH:]
            if d:
                for p in (2 * h, 2 * h + 1):
                    send(part.at[d, p], p1_in.at[k1, p], s_p1.at[d * NP + p], r_p1.at[k1 * NP + p], along1(d))

    for p in range(NP):
        for d in range(1, XN):
            remote(part.at[d, p], p1_in.at[k1s[d], p], s_p1.at[d * NP + p], r_p1.at[k1s[d] * NP + p], partner).wait_recv()
        p2_in[k2, p] = part[0, p] + p1_in[k1s[1], p] + p1_in[k1s[2], p] + p1_in[k1s[3], p]
        for d in order:
            send(p2_in.at[k2, p], p2_in.at[k2, p], s_p2.at[d * NP + p], r_p2.at[k2 * NP + p], along2(d))

    def place(k, p, cc):
        return (p % 2) * BH, pl.multiple_of(cc * (D // 2) + k * OW + (p // 2) * PW, 128)

    def view(k, p, cc):
        r0, c0 = place(k, p, cc)
        return og_v.at[r0:r0 + BH, pl.ds(c0, PW)]

    stores = []

    def store(i, k, p, cc):
        r0, c0 = place(k, p, cc)
        ob_v[i] = og_v[r0:r0 + BH, pl.ds(c0, PW)].astype(BF16)
        cp = pltpu.make_async_copy(ob_v.at[i], out.at[r0:r0 + BH, pl.ds(c0, PW)], sem_out.at[i])
        cp.start()
        stores.append(cp)

    for p in range(NP):
        for d in range(1, XN):
            remote(part.at[d, p], p2_in.at[k2s[d], p], s_p2.at[d * NP + p], r_p2.at[k2s[d] * NP + p], partner).wait_recv()
        r0, c0 = place(k1, p, c)
        tot = p2_in[0, p] + p2_in[1, p] + p2_in[2, p] + p2_in[3, p]
        res = hid_v[:, pl.ds(c0, PW)].astype(F32)[r0:r0 + BH]
        og_v[r0:r0 + BH, pl.ds(c0, PW)] = (res + tot).astype(BF16).astype(F32)
        mine_p = view(k1, p, c)
        for d in order:
            send(mine_p, mine_p, s_ag.at[d * NP + p], r_ag.at[k1 * NP + p], along1(d))
        send(mine_p, mine_p, s_of.at[p], r_of.at[k1 * NP + p], partner)
    for p in range(NP):
        store(p, k1, p, c)
    for p in range(NP):
        for d in order:
            ref = view(k1s[d], p, c)
            remote(ref, ref, s_ag.at[d * NP + p], r_ag.at[k1s[d] * NP + p], partner).wait_recv()
            send(ref, ref, s_of.at[d * NP + p], r_of.at[k1s[d] * NP + p], partner)
            store(d * NP + p, k1s[d], p, c)
    for d in [0] + order:
        for p in range(NP):
            ref = view(k2s[d], p, 1 - c)
            remote(ref, ref, s_of.at[d * NP + p], r_of.at[k2s[d] * NP + p], partner).wait_recv()
            store(XN * NP + d * NP + p, k2s[d], p, 1 - c)
    xe_in = remote(kvn, kv_rcv.at[theirs, :], s_ke.at[0], r_ke.at[0], partner)
    xe_in.wait_recv()
    k_out[...] = kv_rcv[:, 0:strip]
    v_out[...] = kv_rcv[:, strip:2 * strip]
    for cp in qg + kg + cr + sends:
        cp.wait_send()
    for cp in stores:
        cp.wait()


def hand_on(o_in, k_in, v_in, o_out, k_out, v_out, buf, s_in, s_out):
    n, _, w = buf.shape
    reads = [pltpu.make_async_copy(o_in.at[:, i * w:(i + 1) * w], buf.at[i], s_in.at[i]) for i in range(n)]
    writes = [pltpu.make_async_copy(buf.at[i], o_out.at[:, i * w:(i + 1) * w], s_out.at[i]) for i in range(n)]
    for r in reads:
        r.start()
    hd = k_out.shape[2]
    for j in range(k_out.shape[1]):
        k_out[:, j, :] = k_in[:, j * hd:(j + 1) * hd].astype(BF16)
        v_out[:, j, :] = v_in[:, j * hd:(j + 1) * hd].astype(BF16)
    for r, w in zip(reads, writes):
        r.wait()
        w.start()
    for w in writes:
        w.wait()


def solution(mesh):
    TN = mesh.shape['tp']
    SN = mesh.shape['sp']
    XN = SN // 2

    def local_step(hidden, ln_gain, ln_bias, w_q, w_k, w_v, w_o, k_cache, v_cache, lengths):
        B, D = hidden.shape
        _, SL, KVN, HD = k_cache.shape
        G = w_q.shape[1] // (HD * KVN)
        BH = B // 2
        QW = w_q.shape[1] // XN
        KH = D // 2
        KC = 1024
        NQ = KH // KC
        KVR = KH // (XN // 2)
        HB = QW // HD
        OW = D // SN
        PW = OW // 2
        KW = KVN * HD
        assert w_k.shape[1] == KW and KH % KC == 0 and XN == TN == 4 and KVN == 2
        k_t = jnp.transpose(k_cache, (0, 2, 3, 1))
        v_t = jnp.transpose(v_cache, (0, 2, 3, 1))
        gain = ln_gain.reshape(D // 128, 128)
        bias = ln_bias.reshape(D // 128, 128)
        V = pltpu.VMEM
        dma = pltpu.SemaphoreType.DMA
        scratch = [
            V((B, D), BF16), V((2, D // 128, 128), BF16), V((2, D // 128, 128), F32), V((B, KH), BF16), pltpu.SMEM((B,), jnp.int32),
            V((NQ, KC, QW), BF16), V((KVR, KW), BF16), V((XN, QW, OW), BF16),
            V((B, KVN, HD, SL), BF16), V((B, KVN, HD, SL), BF16),
            V((BH, KVN, HD, SL), F32), V((BH, KVN, HD, SL), F32), V((BH, KVN, HD, SL), F32), V((BH, KVN, HD, SL), F32),
            V((B, D), F32), V((2 * XN * 4, BH, PW), BF16), V((B, 2 * KW), F32),
            V((B, QW), F32), V((BH, QW), F32), V((XN, BH, QW), F32), V((2, XN * HB * BH, 128), F32),
            V((B, KW), F32), V((BH, KW), F32), V((XN, BH, KW), F32), V((BH, 2 * KW), F32),
            V((BH, KVN, G, 2 * SL), F32), V((2, XN * HB * BH, 128), F32), V((XN, 2, HB * BH, 128), F32),
            V((BH, QW), F32), V((B, QW), F32), V((XN, 4, BH, PW), F32), V((XN, 4, BH, PW), F32), V((XN, 4, BH, PW), F32),
            dma((4,)), dma((4,)), dma((NQ,)), dma((1,)), dma((XN,)), dma((2 * XN * 4,)),
            dma((2,)), dma((2,)), dma((1,)), dma((1,)), dma((XN,)), dma((XN,)), dma((1,)), dma((1,)), dma((XN,)), dma((XN,)), dma((1,)), dma((1,)),
            dma((XN,)), dma((XN,)), dma((1,)), dma((1,)), dma((XN * 4,)), dma((XN * 4,)), dma((XN * 4,)), dma((XN * 4,)),
            dma((XN * 4,)), dma((XN * 4,)), dma((XN * 4,)), dma((XN * 4,)),
        ]
        cfg = (XN, TN, HD, G, KC, HD ** -0.5)
        out, k_new, v_new = pl.pallas_call(
            functools.partial(kernel, cfg),
            out_shape=(jax.ShapeDtypeStruct((B, D), BF16), jax.ShapeDtypeStruct((B, KW), F32), jax.ShapeDtypeStruct((B, KW), F32)),
            in_specs=[pl.BlockSpec(memory_space=pl.ANY)] * 10,
            out_specs=(pl.BlockSpec(memory_space=pl.ANY),) + (pl.BlockSpec(memory_space=pltpu.VMEM),) * 2,
            scratch_shapes=scratch,
            compiler_params=pltpu.CompilerParams(collective_id=0, has_side_effects=True, vmem_limit_bytes=67043328),
            name='decode_step',
        )(hidden, gain, bias, w_q, w_k, w_v, w_o, k_t, v_t, lengths)
        vm = pl.BlockSpec(memory_space=pltpu.VMEM)
        hb = pl.BlockSpec(memory_space=pl.ANY)
        head = jax.ShapeDtypeStruct((B, KVN, HD), BF16)
        return pl.pallas_call(
            hand_on, out_shape=(jax.ShapeDtypeStruct((B, D), BF16), head, head), in_specs=[hb, vm, vm], out_specs=(hb, vm, vm),
            scratch_shapes=[V((4, B, D // 4), BF16), dma((4,)), dma((4,))], name='hand_on')(out, k_new, v_new)

    row_spec = P('dp', None)
    cache_spec = P('dp', 'sp', 'tp', None)
    head_spec = P('dp', 'tp', None)
    return jax.shard_map(local_step, mesh=mesh, in_specs=(row_spec, P(None), P(None), P(None, 'tp'), P(None, 'tp'), P(None, 'tp'), P('tp', None), cache_spec, cache_spec, P('dp')), out_specs=(row_spec, head_spec, head_spec), check_vma=False)
```

```python
import functools

import jax
import jax.numpy as jnp
from jax import lax
from jax.experimental import pallas as pl
from jax.experimental.pallas import tpu as pltpu
from jax.sharding import PartitionSpec as P

F32 = jnp.float32
BF16 = jnp.bfloat16
MESH_ID = pl.DeviceIdType.MESH


def dot(a, b):
    return jnp.dot(a, b, preferred_element_type=F32)


def dot_t(a, b):
    return lax.dot_general(a, b, (((1,), (1,)), ((), ())), preferred_element_type=F32)


def rope(u, cos_t, sin_lo, sin_hi, half):
    width = u.shape[1]
    ahead = pltpu.roll(u, width - half, 1)
    behind = pltpu.roll(u, half, 1)
    return u * cos_t + ahead * sin_lo + behind * sin_hi


def kernel(cfg, hidden, gain, bias, w_q, w_k, w_v, w_o, k_t, v_t, lens, out, k_out, v_out,
           hid_v, gb_raw, gb_f, h_v, len_s, wq_v, wkv_v, wo_v, kc_v, vc_v, k_snd, v_snd, k_rcv, v_rcv,
           og_v, ob_v, kv_rcv, qp, q_in, q_all, qh, kvp, kv_in, kv_all, kvn, score, ob, o_in, ctx_own, ctx_all, part, p1_in, p2_in,
           sem_small, sem_cache, sem_wq, sem_wkv, sem_wo, sem_out,
           s_cx, r_cx, s_qd, r_qd, s_qg, r_qg, s_kd, r_kd, s_kg, r_kg, s_ke, r_ke,
           s_cr, r_cr, s_cf, r_cf, s_p1, r_p1, s_p2, r_p2, s_ag, r_ag, s_of, r_of):
    XN, TN, HD, G, KC, scale = cfg
    B, D = hidden.shape
    BH = B // 2
    SL = k_t.shape[3]
    KVN = k_t.shape[1]
    QW = w_q.shape[1] // XN
    KH = D // 2
    KVR = KH // (XN // 2)
    HB = QW // HD
    OW = D // (2 * XN)
    NH = 3
    PW = OW // NH
    NP = 2 * NH
    rot = HD // 2
    half = rot // 2
    strip = 2 * HD
    RB = HB * BH

    t = lax.axis_index('tp')
    s = lax.axis_index('sp')
    x = s // 2
    c = s % 2
    other = s + 1 - 2 * c
    xs = [(x + d) % XN for d in range(XN)]
    ts = [(t + d) % TN for d in range(TN)]
    partner = {'sp': other}

    def xpeer(d):
        return {'sp': 2 * xs[d] + c}

    def remote(src, dst, ss, rs, dev):
        return pltpu.make_async_remote_copy(src_ref=src, dst_ref=dst, send_sem=ss, recv_sem=rs, device_id=dev, device_id_type=MESH_ID)

    mine = pl.ds(pl.multiple_of(c * BH, BH), BH)
    theirs = pl.ds(pl.multiple_of((1 - c) * BH, BH), BH)

    c_hid = pltpu.make_async_copy(hidden, hid_v, sem_small.at[0])
    c_gain = pltpu.make_async_copy(gain, gb_raw.at[0], sem_small.at[1])
    c_bias = pltpu.make_async_copy(bias, gb_raw.at[1], sem_small.at[2])
    c_len = pltpu.make_async_copy(lens, len_s, sem_small.at[3])
    for cp in (c_hid, c_gain, c_bias, c_len):
        cp.start()
    c_cache = [pltpu.make_async_copy(k_t.at[theirs], kc_v.at[theirs], sem_cache.at[0]),
               pltpu.make_async_copy(v_t.at[theirs], vc_v.at[theirs], sem_cache.at[1]),
               pltpu.make_async_copy(k_t.at[mine], kc_v.at[mine], sem_cache.at[2]),
               pltpu.make_async_copy(v_t.at[mine], vc_v.at[mine], sem_cache.at[3])]
    qcol = pl.ds(pl.multiple_of(x * QW, 128), QW)
    NQ = KH // KC

    def wq_copy(i):
        return pltpu.make_async_copy(w_q.at[pl.ds(pl.multiple_of(c * KH + i * KC, KC), KC), qcol], wq_v.at[i], sem_wq.at[i])

    c_cache[0].start()
    c_cache[1].start()
    wq_copy(0).start()
    wq_copy(1).start()
    kvrow = pl.ds(pl.multiple_of(c * KH + (x % (XN // 2)) * KVR, KVR), KVR)
    c_wk = pltpu.make_async_copy(w_k.at[kvrow, :], wkv_v, sem_wkv.at[0])
    c_wv = pltpu.make_async_copy(w_v.at[kvrow, :], wkv_v, sem_wkv.at[0])

    def start_wkv():
        @pl.when(x < XN // 2)
        def _():
            c_wk.start()

        @pl.when(x >= XN // 2)
        def _():
            c_wv.start()

    axis = [(c + h) % 2 for h in range(NH)]
    k1 = [x * (1 - a) + t * a for a in axis]
    k2 = [x * a + t * (1 - a) for a in axis]

    def along1(h, d):
        return {'tp': (t + axis[h] * d) % TN, 'sp': 2 * ((x + (1 - axis[h]) * d) % XN) + c}

    def along2(h, d):
        return {'tp': (t + (1 - axis[h]) * d) % TN, 'sp': 2 * ((x + axis[h] * d) % XN) + c}

    def wo_copy(h, d):
        cols = pl.ds(pl.multiple_of(c * (D // 2) + (k1[h] + d) % XN * OW + h * PW, 128), PW)
        return pltpu.make_async_copy(w_o.at[pl.ds(pl.multiple_of(x * QW, QW), QW), cols], wo_v.at[h, d], sem_wo.at[h * XN + d])

    order = [1, XN - 1] + list(range(2, XN - 1))
    later = [functools.partial(lambda i: wq_copy(i).start(), i) for i in range(2, NQ)]
    later += [start_wkv, c_cache[2].start, c_cache[3].start]
    far_first = [2, 1, 3, 0]
    later += [functools.partial(lambda h, d: wo_copy(h, d).start(), h, d) for h in range(NH) for d in far_first]

    def issue(n):
        for _ in range(n):
            if later:
                later.pop(0)()

    barrier = pltpu.get_barrier_semaphore()
    pl.semaphore_signal(barrier, inc=1, device_id=partner, device_id_type=MESH_ID)
    for dx in range(XN):
        for dt in range(TN):
            if dx or dt:
                pl.semaphore_signal(barrier, inc=1, device_id={'tp': ts[dt], 'sp': 2 * xs[dx] + c}, device_id_type=MESH_ID)

    c_hid.wait()
    nt = D // 128
    UN = 8

    def sum_step(i, a):
        for u in range(UN):
            a = a + hid_v[:, pl.ds(pl.multiple_of((i * UN + u) * 128, 128), 128)].astype(F32)
        return a

    tot = lax.fori_loop(0, nt // UN, sum_step, jnp.zeros((B, 128), F32))
    mean = jnp.sum(tot, axis=1, keepdims=True) / D

    def var_step(i, a):
        for u in range(UN):
            v = hid_v[:, pl.ds(pl.multiple_of((i * UN + u) * 128, 128), 128)].astype(F32) - mean
            a = a + v * v
        return a

    sq = lax.fori_loop(0, nt // UN, var_step, jnp.zeros((B, 128), F32))
    issue(1)
    rstd = lax.rsqrt(jnp.sum(sq, axis=1, keepdims=True) / D + 1e-5)
    c_gain.wait()
    c_bias.wait()
    issue(1)
    gb_f[0] = 1.0 + gb_raw[0].astype(F32)
    gb_f[1] = gb_raw[1].astype(F32)

    def norm_step(i, _):
        for u in range(UN):
            j = i * UN + u
            col = c * (nt // 2) + j
            v = hid_v[:, pl.ds(pl.multiple_of(col * 128, 128), 128)].astype(F32)
            v = (v - mean) * rstd * gb_f[0, pl.ds(col, 1), :] + gb_f[1, pl.ds(col, 1), :]
            h_v[:, pl.ds(pl.multiple_of(j * 128, 128), 128)] = v.astype(BF16)
        return 0

    lax.fori_loop(0, nt // 2 // UN, norm_step, 0)

    c_len.wait()
    row = lax.broadcasted_iota(jnp.int32, (BH, strip), 0)
    lane = lax.broadcasted_iota(jnp.int32, (BH, strip), 1)
    pos = jnp.zeros((BH, strip), F32)
    for r in range(BH):
        pos = jnp.where(row == r, len_s[c * BH + r].astype(F32), pos)
    hl = jnp.where(lane >= HD, lane - HD, lane)
    il = jnp.where(hl >= half, hl - half, hl)
    freq = jnp.exp(il.astype(F32) * (-2.0 / rot * 9.210340371976184))
    ang = jnp.where(hl < rot, pos * freq, 0.0)
    cos_t = jnp.cos(ang)
    sin_t = jnp.sin(ang)
    sin_lo = jnp.where(hl < half, -sin_t, 0.0)
    sin_hi = jnp.where(hl >= half, sin_t, 0.0)

    pl.semaphore_wait(barrier, XN * TN)

    c_cache[0].wait()
    c_cache[1].wait()

    def widen(b, _):
        k_snd[b] = kc_v[(1 - c) * BH + b].astype(F32)
        v_snd[b] = vc_v[(1 - c) * BH + b].astype(F32)
        return 0

    lax.fori_loop(0, BH, widen, 0)
    xk = remote(k_snd, k_rcv, s_cx.at[0], r_cx.at[0], partner)
    xv = remote(v_snd, v_rcv, s_cx.at[1], r_cx.at[1], partner)
    xk.start()
    xv.start()

    a = None
    for i in range(NQ):
        wq_copy(i).wait()
        issue(1)
        r = dot(h_v[:, i * KC:(i + 1) * KC], wq_v[i])
        a = r if a is None else a + r
    issue(len(later))
    qp[...] = a
    xq = remote(qp.at[theirs, :], q_in, s_qd.at[0], r_qd.at[0], partner)
    xq.start()

    xq.wait()
    qb = qp[mine, :] + q_in[...]
    for i in range(QW // strip):
        sl = slice(i * strip, (i + 1) * strip)
        q_all[x, :, sl] = rope(qb[:, sl], cos_t, sin_lo, sin_hi, half).astype(BF16).astype(F32)
    for d in far_first[:3]:
        remote(q_all.at[x], q_all.at[x], s_qg.at[0], r_qg.at[0], xpeer(d)).start()

    @pl.when(x < XN // 2)
    def _():
        c_wk.wait()

    @pl.when(x >= XN // 2)
    def _():
        c_wv.wait()

    kvp[...] = dot(h_v[:, pl.ds(pl.multiple_of((x % (XN // 2)) * KVR, KVR), KVR)], wkv_v[...])
    xkd = remote(kvp.at[theirs, :], kv_in, s_kd.at[0], r_kd.at[0], partner)
    xkd.start()
    xkd.wait()
    kv_all[x] = kvp[mine, :] + kv_in[...]
    for d in range(1, XN):
        remote(kv_all.at[x], kv_all.at[x], s_kg.at[0], r_kg.at[0], xpeer(d)).start()

    group = q_all.at[0:XN - 1]
    remote(group, group, s_qg.at[0], r_qg.at[0], partner).wait_recv()
    for blk in range(XN):
        for j in range(HB):
            h = blk * HB + j
            v = q_all[blk, :, j * HD:(j + 1) * HD]
            qh[0, h * BH:(h + 1) * BH, :] = v[:, 0:128]
            qh[1, h * BH:(h + 1) * BH, 0:HD - 128] = v[:, 128:HD]

    c_cache[2].wait()
    c_cache[3].wait()
    xk.wait()
    xv.wait()
    lane2 = lax.broadcasted_iota(jnp.int32, (G, 2 * SL), 1)
    p_here = jnp.where(lane2 < SL, s * SL + lane2, other * SL + lane2 - SL)
    for b in range(BH):
        for kv in range(KVN):
            rows = pl.ds(kv * G * BH + b, G, stride=BH)
            q = jnp.concatenate([qh[0, rows, :], qh[1, rows, :]], axis=1)[:, 0:HD].astype(BF16)
            s0 = dot(q, kc_v[c * BH + b, kv])
            s1 = dot(q, k_rcv[b, kv].astype(BF16))
            score[b, kv] = jnp.concatenate([s0, s1], axis=1)
    neg = -jnp.inf

    tail_lane = lax.broadcasted_iota(jnp.int32, (G, 128), 1)
    for b in range(BH):
        n = len_s[c * BH + b]
        for kv in range(KVN):
            sc = jnp.where(p_here < n, score[b, kv] * scale, neg)
            m = jnp.max(sc, axis=1, keepdims=True)
            ms = jnp.where(m == neg, 0.0, m)
            w = jnp.exp(sc - ms)
            l = jnp.sum(w, axis=1, keepdims=True)
            wb = w.astype(BF16)
            pv = dot_t(wb[:, 0:SL], vc_v[c * BH + b, kv]) + dot_t(wb[:, SL:], v_rcv[b, kv].astype(BF16))
            tail = jnp.concatenate([pv[:, 128:HD], jnp.zeros((G, 256 - HD), F32)], axis=1)
            tail = jnp.where(tail_lane == HD - 128, m, jnp.where(tail_lane == HD - 127, l, tail))
            rows = pl.ds(kv * G * BH + b, G, stride=BH)
            ob[0, rows, :] = pv[:, 0:128]
            ob[1, rows, :] = tail

    for d in far_first[:3]:
        remote(ob.at[:, pl.ds(pl.multiple_of(xs[d] * RB, RB), RB), :], o_in.at[x], s_cr.at[0], r_cr.at[0], xpeer(d)).start()

    group = kv_all.at[0:XN - 1]
    remote(group, group, s_kg.at[0], r_kg.at[0], partner).wait_recv()
    kn = kv_all[0]
    vn = kv_all[XN // 2]
    for i in range(1, XN // 2):
        kn = kn + kv_all[i]
        vn = vn + kv_all[XN // 2 + i]
    kn = rope(kn, cos_t, sin_lo, sin_hi, half).astype(BF16).astype(F32)
    vn = vn.astype(BF16).astype(F32)
    kvn[:, 0:strip] = kn
    kvn[:, strip:2 * strip] = vn
    kv_rcv[mine, :] = kvn[...]
    xe = remote(kvn, kv_rcv.at[mine, :], s_ke.at[0], r_ke.at[0], partner)
    xe.start()
    second = x >= XN // 2
    kh = jnp.where(second, kn[:, HD:], kn[:, 0:HD])
    vh = jnp.where(second, vn[:, HD:], vn[:, 0:HD])

    own = pl.ds(pl.multiple_of(x * RB, RB), RB)
    q_own = jnp.concatenate([qh[0, own, :], qh[1, own, :]], axis=1)[:, 0:HD]
    k_rep = jnp.concatenate([kh] * HB, axis=0)
    v_rep = jnp.concatenate([vh] * HB, axis=0)
    self_s = jnp.sum(q_own * k_rep, axis=1, keepdims=True) * scale
    group = o_in.at[0:XN - 1]
    remote(group, group, s_cr.at[0], r_cr.at[0], partner).wait_recv()
    o_in[x] = ob[:, own, :]
    parts = [jnp.concatenate([o_in[i, 0], o_in[i, 1]], axis=1) for i in range(XN)]
    ms = [p[:, HD:HD + 1] for p in parts]
    ls = [p[:, HD + 1:HD + 2] for p in parts]
    top = self_s
    for m in ms:
        top = jnp.maximum(top, m)
    f_self = jnp.exp(self_s - top)
    num = f_self * v_rep
    den = f_self
    for p, m, l in zip(parts, ms, ls):
        f = jnp.exp(m - top)
        num = num + f * p[:, 0:HD]
        den = den + f * l
    ctx = (num / den).astype(BF16).astype(F32)
    for j in range(HB):
        ctx_own[:, j * HD:(j + 1) * HD] = ctx[j * BH:(j + 1) * BH, :]

    ctx_all[mine, :] = ctx_own[...]
    cf = remote(ctx_own, ctx_all.at[mine, :], s_cf.at[0], r_cf.at[0], partner)
    cf.start()
    remote(ctx_own, ctx_all.at[theirs, :], s_cf.at[0], r_cf.at[0], partner).wait_recv()

    lhs = ctx_all[...].astype(BF16)
    sends = [xe, cf]

    def send(src, dst, ss, rs, dev):
        cp = remote(src, dst, ss, rs, dev)
        cp.start()
        sends.append(cp)

    for h in range(NH):
        for d in far_first:
            wo_copy(h, d).wait()
    for h in range(NH):
        for d in far_first:
            r = dot(lhs, wo_v[h, d])
            for p in (2 * h, 2 * h + 1):
                part[d, p] = r[(p % 2) * BH:(p % 2 + 1) * BH]
                if d:
                    send(part.at[d, p], p1_in.at[k1[h], p], s_p1.at[0], r_p1.at[p], along1(h, d))

    remote(kvn, kv_rcv.at[theirs, :], s_ke.at[0], r_ke.at[0], partner).wait_recv()
    stores = [pltpu.make_async_copy(kv_rcv.at[:, 0:strip], k_out, sem_small.at[0]),
              pltpu.make_async_copy(kv_rcv.at[:, strip:2 * strip], v_out, sem_small.at[1])]
    for cp in stores:
        cp.start()

    for p in range(NP):
        group = p1_in.at[0:XN - 1, p]
        remote(group, group, s_p1.at[0], r_p1.at[p], partner).wait_recv()
        h = p // 2
        p2_in[k2[h], p] = part[0, p] + p1_in[(k1[h] + 1) % XN, p] + p1_in[(k1[h] + 2) % XN, p] + p1_in[(k1[h] + 3) % XN, p]
        for d in order:
            send(p2_in.at[k2[h], p], p2_in.at[k2[h], p], s_p2.at[0], r_p2.at[p], along2(h, d))

    def place(k, p, cc):
        return (p % 2) * BH, pl.multiple_of(cc * (D // 2) + k * OW + (p // 2) * PW, 128)

    def view(k, p, cc):
        r0, c0 = place(k, p, cc)
        return og_v.at[r0:r0 + BH, pl.ds(c0, PW)]

    def store(i, k, p, cc):
        r0, c0 = place(k, p, cc)
        ob_v[i] = og_v[r0:r0 + BH, pl.ds(c0, PW)].astype(BF16)
        cp = pltpu.make_async_copy(ob_v.at[i], out.at[r0:r0 + BH, pl.ds(c0, PW)], sem_out.at[0])
        cp.start()

    for p in range(NP):
        group = p2_in.at[0:XN - 1, p]
        remote(group, group, s_p2.at[0], r_p2.at[p], partner).wait_recv()
        h = p // 2
        r0, c0 = place(k1[h], p, c)
        tot = p2_in[0, p] + p2_in[1, p] + p2_in[2, p] + p2_in[3, p]
        res = hid_v[:, pl.ds(c0, PW)].astype(F32)[r0:r0 + BH]
        og_v[r0:r0 + BH, pl.ds(c0, PW)] = (res + tot).astype(BF16).astype(F32)
        mine_p = view(k1[h], p, c)
        for d in order:
            send(mine_p, mine_p, s_ag.at[0], r_ag.at[p], along1(h, d))
        send(mine_p, mine_p, s_of.at[0], r_of.at[p], partner)
    for p in range(NP):
        store(p, k1[p // 2], p, c)
    for p in range(NP):
        group = p1_in.at[0:XN - 1, p]
        remote(group, group, s_ag.at[0], r_ag.at[p], partner).wait_recv()
        for d in order:
            ref = view((k1[p // 2] + d) % XN, p, c)
            send(ref, ref, s_of.at[0], r_of.at[p], partner)
        for d in order:
            store(d * NP + p, (k1[p // 2] + d) % XN, p, c)
    for p in range(NP):
        group = p1_in.at[:, p]
        remote(group, group, s_of.at[0], r_of.at[p], partner).wait_recv()
        for k in range(XN):
            store(XN * NP + k * NP + p, k, p, 1 - c)
    for cp in (xe, cf):
        cp.wait_send()
    for group, sem in ((q_all.at[0:XN - 1], s_qg), (kv_all.at[0:XN - 1], s_kg), (o_in.at[0:XN - 1], s_cr), (p1_in.at[0:XN - 1], s_p1),
                       (p1_in.at[0:XN - 1], s_p2), (p1_in.at[0:XN - 1], s_ag), (p1_in, s_of)):
        remote(group, group, sem.at[0], r_qg.at[0], partner).wait_send()
    for cp in stores + [pltpu.make_async_copy(hid_v, out, sem_out.at[0])]:
        cp.wait()


def hand_on(o_in, k_in, v_in, o_out, k_out, v_out, buf, kv_f, kv_b, s_in, s_out):
    n, _, w = buf.shape
    reads = [pltpu.make_async_copy(o_in.at[:, i * w:(i + 1) * w], buf.at[i], s_in.at[i]) for i in range(n)]
    writes = [pltpu.make_async_copy(buf.at[i], o_out.at[:, i * w:(i + 1) * w], s_out.at[i]) for i in range(n)]
    kv_reads = [pltpu.make_async_copy(src, kv_f.at[i], s_in.at[n + i]) for i, src in enumerate((k_in, v_in))]
    kv_writes = [pltpu.make_async_copy(kv_b.at[i], dst, s_out.at[n + i]) for i, dst in enumerate((k_out, v_out))]
    for r in kv_reads + reads:
        r.start()
    hd = k_out.shape[2]
    for i in range(2):
        kv_reads[i].wait()
        for j in range(k_out.shape[1]):
            kv_b[i, :, j, :] = kv_f[i, :, j * hd:(j + 1) * hd].astype(BF16)
        kv_writes[i].start()
    for r, w in zip(reads, writes):
        r.wait()
        w.start()
    for w in kv_writes + writes:
        w.wait()


def solution(mesh):
    TN = mesh.shape['tp']
    SN = mesh.shape['sp']
    XN = SN // 2

    def local_step(hidden, ln_gain, ln_bias, w_q, w_k, w_v, w_o, k_cache, v_cache, lengths):
        B, D = hidden.shape
        _, SL, KVN, HD = k_cache.shape
        G = w_q.shape[1] // (HD * KVN)
        BH = B // 2
        QW = w_q.shape[1] // XN
        KH = D // 2
        KC = 1024
        NQ = KH // KC
        KVR = KH // (XN // 2)
        HB = QW // HD
        OW = D // SN
        PW = OW // 3
        KW = KVN * HD
        assert w_k.shape[1] == KW and KH % KC == 0 and XN == TN == 4 and KVN == 2
        k_t = jnp.transpose(k_cache, (0, 2, 3, 1))
        v_t = jnp.transpose(v_cache, (0, 2, 3, 1))
        gain = ln_gain.reshape(D // 128, 128)
        bias = ln_bias.reshape(D // 128, 128)
        V = pltpu.VMEM
        dma = pltpu.SemaphoreType.DMA
        scratch = [
            V((B, D), BF16), V((2, D // 128, 128), BF16), V((2, D // 128, 128), F32), V((B, KH), BF16), pltpu.SMEM((B,), jnp.int32),
            V((NQ, KC, QW), BF16), V((KVR, KW), BF16), V((3, XN, QW, PW), BF16),
            V((B, KVN, HD, SL), BF16), V((B, KVN, HD, SL), BF16),
            V((BH, KVN, HD, SL), F32), V((BH, KVN, HD, SL), F32), V((BH, KVN, HD, SL), F32), V((BH, KVN, HD, SL), F32),
            V((B, D), F32), V((2 * XN * 6, BH, PW), BF16), V((B, 2 * KW), F32),
            V((B, QW), F32), V((BH, QW), F32), V((XN, BH, QW), F32), V((2, XN * HB * BH, 128), F32),
            V((B, KW), F32), V((BH, KW), F32), V((XN, BH, KW), F32), V((BH, 2 * KW), F32),
            V((BH, KVN, G, 2 * SL), F32), V((2, XN * HB * BH, 128), F32), V((XN, 2, HB * BH, 128), F32),
            V((BH, QW), F32), V((B, QW), F32), V((XN, 6, BH, PW), F32), V((XN, 6, BH, PW), F32), V((XN, 6, BH, PW), F32),
            dma((4,)), dma((4,)), dma((NQ,)), dma((1,)), dma((3 * XN,)), dma((1,)),
            dma((2,)), dma((2,)), dma((1,)), dma((1,)), dma((1,)), dma((1,)), dma((1,)), dma((1,)), dma((1,)), dma((1,)), dma((1,)), dma((1,)),
            dma((1,)), dma((1,)), dma((1,)), dma((1,)), dma((1,)), dma((6,)), dma((1,)), dma((6,)), dma((1,)), dma((6,)), dma((1,)), dma((6,)),
        ]
        cfg = (XN, TN, HD, G, KC, HD ** -0.5)
        out, k_new, v_new = pl.pallas_call(
            functools.partial(kernel, cfg),
            out_shape=(jax.ShapeDtypeStruct((B, D), BF16), jax.ShapeDtypeStruct((B, KW), F32), jax.ShapeDtypeStruct((B, KW), F32)),
            in_specs=[pl.BlockSpec(memory_space=pl.ANY)] * 10,
            out_specs=(pl.BlockSpec(memory_space=pl.ANY),) * 3,
            scratch_shapes=scratch,
            compiler_params=pltpu.CompilerParams(collective_id=0, has_side_effects=True, vmem_limit_bytes=67043328),
            name='decode_step',
        )(hidden, gain, bias, w_q, w_k, w_v, w_o, k_t, v_t, lengths)
        hb = pl.BlockSpec(memory_space=pl.ANY)
        head = jax.ShapeDtypeStruct((B, KVN, HD), BF16)
        return pl.pallas_call(
            hand_on, out_shape=(jax.ShapeDtypeStruct((B, D), BF16), head, head), in_specs=[hb] * 3, out_specs=(hb,) * 3,
            scratch_shapes=[V((2, B, D // 2), BF16), V((2, B, KW), F32), V((2, B, KVN, HD), BF16), dma((4,)), dma((4,))], name='hand_on')(out, k_new, v_new)

    row_spec = P('dp', None)
    cache_spec = P('dp', 'sp', 'tp', None)
    head_spec = P('dp', 'tp', None)
    return jax.shard_map(local_step, mesh=mesh, in_specs=(row_spec, P(None), P(None), P(None, 'tp'), P(None, 'tp'), P(None, 'tp'), P('tp', None), cache_spec, cache_spec, P('dp')), out_specs=(row_spec, head_spec, head_spec), check_vma=False)
```
